32 devices in a mesh: gene: 8 (over z, x), cell: 4 (over y, core).
Axes of the slice: x: 2, y: 2, z: 4, core: 2. Of those that a mesh axis runs over, the one named last changes fastest.
Arguments:
- counts: bfloat16 [32768, 8192], P('gene', 'cell'), may hold values from -6 to 6
- loadings: float32 [32768, 128], P('gene'), may hold values from -0.03125 to 0.03125
- values: float32 [128], replicated, may hold values from 0.5 to 2
- test_matrix: bfloat16 [8192, 128], P('cell'), may hold values from -0.0625 to 0.0625
- tile_mask: int32 [128, 64], P('gene', 'cell'), may hold values 0 or 1
Outputs:
- new_loadings: float32 [32768, 128], P('gene')
- new_values: float32 [128], replicated
The draws below stay inside these ranges and needn't reach their ends.
All inputs are finite; a program needn't handle non-finite values. No bound on the sum of `tile_mask` on one device may be relied on, other than what follows from the above.
Results may differ from the reference program's by a relative error of at most 0.0028.
Values sent between devices are 32-bit elements; how exact they have to be, the bound alone decides.
A program may use at most 128 MiB of HBM per device.

```python
import math
import jax
import jax.numpy as jnp
from jax import lax

GENES = 32768
COMPONENTS = 128
SKETCH = 128
GENE_TILE = 256
CELL_TILE = 128
SWEEPS = 3
CELLS = 8192
N_GENE = 8


def touch_ends(entries, rng, low, high):
    dims = entries.shape
    index_at = [jax.random.randint(jax.random.fold_in(rng, axis), (), 0, dims[axis]) for axis in range(len(dims))]
    entries = entries.at[tuple(index_at)].set(low)
    longest = dims.index(max(dims))
    index_at[longest] = (index_at[longest] + 1) % dims[longest]
    return entries.at[tuple(index_at)].set(high)


def levels(rng, extent, shards, low, top_value):
    loudness = 1.0
    for position, parts in shards:
        heights = jax.random.uniform(jax.random.fold_in(jax.random.fold_in(rng, 6), position), (parts,), jnp.float32, low / len(shards), top_value / len(shards))
        loudness = loudness * jnp.repeat(jnp.exp(heights), extent[position] // parts).reshape((-1,) + (1,) * (len(extent) - 1 - position))
    return loudness


def gaussian(rng, dims, deviation, limit, shards=(), kind=jnp.bfloat16):
    factor_of = levels(rng, dims, shards, -0.22, 0.18) if shards else 1.0
    drawn = jax.random.normal(rng, dims, jnp.float32) * deviation * factor_of
    return jnp.minimum(jnp.maximum(drawn, -limit), limit).astype(kind)


def setup_inputs(seed: int = 0) -> dict:
    key_of = jax.random.split(jax.random.key(seed), 6)
    counts = gaussian(key_of[0], (GENES, CELLS), 1.0, 6.0, ((0, 8), (1, 4)))
    loadings = gaussian(key_of[1], (GENES, COMPONENTS), GENES ** -0.5, 0.03125, ((0, 8),), jnp.float32)
    values = jnp.clip(jnp.exp(jax.random.uniform(key_of[2], (COMPONENTS,), jnp.float32, math.log(0.5), math.log(2.0))), 0.5, 2.0)
    test_matrix = gaussian(key_of[3], (CELLS, SKETCH), CELLS ** -0.5, 0.0625, ((0, 4),))
    tile_mask = touch_ends((jax.random.randint(key_of[4], (GENES // GENE_TILE, CELLS // CELL_TILE), 0, 4) < 3).astype(jnp.int32), jax.random.fold_in(key_of[4], 1), 0, 1)
    return {"counts": counts, "loadings": loadings, "values": values, "test_matrix": test_matrix, "tile_mask": tile_mask}


def masked_block(count_block, tile_block):
    tile_wide = jnp.repeat(jnp.repeat(tile_block.astype(jnp.bfloat16), GENE_TILE, axis=0), CELL_TILE, axis=1)
    return count_block * tile_wide

def reference(counts, loadings, values, test_matrix, tile_mask):
    highest = lax.Precision.HIGHEST
    gene_rows = GENES // N_GENE
    count_blocks = counts.reshape(N_GENE, gene_rows, CELLS)
    load_blocks = loadings.reshape(N_GENE, gene_rows, COMPONENTS)
    tile_blocks = tile_mask.reshape(N_GENE, gene_rows // GENE_TILE, CELLS // CELL_TILE)

    def project_step(running, inputs):
        count_block, load_block, tile_block = inputs
        masked = masked_block(count_block, tile_block)
        return (running + jnp.dot(load_block.astype(jnp.bfloat16).T.astype(jnp.float32), masked.astype(jnp.float32), preferred_element_type=jnp.float32), None)
    projection, unused = lax.scan(project_step, jnp.zeros((COMPONENTS, CELLS), jnp.float32), (count_blocks, load_blocks, tile_blocks))
    test_wide = test_matrix.astype(jnp.float32)

    def residual_of(count_block, load_block, tile_block):
        masked = masked_block(count_block, tile_block)
        return masked.astype(jnp.float32) - jnp.dot(load_block, projection, precision=highest)

    def sketch_step(inputs):
        count_block, load_block, tile_block = inputs
        return jnp.dot(residual_of(count_block, load_block, tile_block), test_wide, precision=highest)
    sketch = lax.map(sketch_step, (count_blocks, load_blocks, tile_blocks)).reshape(GENES, SKETCH)
    sketch_gram = jnp.dot(sketch.T, sketch, precision=highest)
    factor = jnp.linalg.cholesky(sketch_gram)
    basis = jax.scipy.linalg.solve_triangular(factor, sketch.T, lower=True).T
    basis_blocks = basis.reshape(N_GENE, gene_rows, SKETCH)

    def coef_step(running, inputs):
        count_block, load_block, tile_block, basis_block = inputs
        residual = residual_of(count_block, load_block, tile_block)
        return (running + jnp.dot(basis_block.T, residual, precision=highest), None)
    coef, unused = lax.scan(coef_step, jnp.zeros((SKETCH, CELLS), jnp.float32), (count_blocks, load_blocks, tile_blocks, basis_blocks))
    stacked = jnp.concatenate([projection, coef], axis=0)
    squares = jnp.concatenate([values * values, jnp.zeros((SKETCH,), jnp.float32)])
    core_matrix = jnp.dot(stacked, stacked.T, precision=highest) / CELLS + jnp.diag(squares)
    subspace = jnp.eye(COMPONENTS + SKETCH, COMPONENTS, dtype=jnp.float32)
    for sweep in range(SWEEPS):
        image_block = jnp.dot(core_matrix, subspace, precision=highest)
        chol = jnp.linalg.cholesky(jnp.dot(image_block.T, image_block, precision=highest))
        subspace = jax.scipy.linalg.solve_triangular(chol, image_block.T, lower=True).T
    final_image = jnp.dot(core_matrix, subspace, precision=highest)
    new_values = jnp.sqrt(lax.optimization_barrier(jnp.sum(subspace * final_image, axis=0)))
    rotated = jnp.dot(loadings, subspace[:COMPONENTS], precision=highest) + jnp.dot(basis, subspace[COMPONENTS:], precision=highest)
    new_loadings = rotated * GENES ** 0.5
    return (new_loadings, new_values)
```

```python
import functools

import jax
import jax.numpy as jnp
from jax import lax
from jax.experimental import pallas as pl
from jax.experimental.pallas import tpu as pltpu
from jax.sharding import PartitionSpec as P

GENE_TILE = 256
CELL_TILE = 128
SWEEPS = 3
ROW_BLOCK = 512
CHUNKS = 8
HIGH = lax.Precision.HIGHEST
MESH = pl.DeviceIdType.MESH
LIMIT = 60 * 1024 * 1024
VMEM = pl.BlockSpec(memory_space=pltpu.VMEM)


def dot(a, b, dims=((1,), (0,)), precision=HIGH):
    return lax.dot_general(
        a, b, (dims, ((), ())), precision=precision, preferred_element_type=jnp.float32
    )


def split(a):
    high = a.astype(jnp.bfloat16)
    return high, (a - high.astype(jnp.float32)).astype(jnp.bfloat16)


def masked_rows(counts_ref, mask_ref, step):
    parts = []
    per_block = ROW_BLOCK // GENE_TILE
    for part in range(per_block):
        row = mask_ref[step * per_block + part].astype(jnp.bfloat16)
        parts.append(counts_ref[pl.ds(part * GENE_TILE, GENE_TILE), :] * row)
    return jnp.concatenate(parts, axis=0)


def first_kernel(counts_ref, mask_ref, load_ref, test_ref, y_ref, p_ref, z_ref):
    step = pl.program_id(0)
    masked = masked_rows(counts_ref, mask_ref, step)
    y_ref[...] = dot(masked, test_ref[...], precision=None)
    part = dot(load_ref[...].astype(jnp.bfloat16), masked, ((0,), (0,)), None)

    @pl.when(step == 0)
    def _():
        p_ref[...] = part

    @pl.when(step > 0)
    def _():
        p_ref[...] += part

    @pl.when(step == pl.num_programs(0) - 1)
    def _():
        high, low = split(p_ref[...])
        z_ref[...] = dot(high, test_ref[...], precision=None) + dot(
            low, test_ref[...], precision=None
        )


def first_pass(counts, mask_rows, loadings, test_matrix):
    rows, cols = counts.shape
    comps, width = loadings.shape[1], test_matrix.shape[1]
    return pl.pallas_call(
        first_kernel,
        grid=(rows // ROW_BLOCK,),
        in_specs=[
            pl.BlockSpec((ROW_BLOCK, cols), lambda i: (i, 0)),
            pl.BlockSpec(mask_rows.shape, lambda i: (0, 0, 0)),
            pl.BlockSpec((ROW_BLOCK, comps), lambda i: (i, 0)),
            pl.BlockSpec(test_matrix.shape, lambda i: (0, 0)),
        ],
        out_specs=[
            pl.BlockSpec((ROW_BLOCK, width), lambda i: (i, 0)),
            pl.BlockSpec((comps, cols), lambda i: (0, 0)),
            pl.BlockSpec((comps, width), lambda i: (0, 0)),
        ],
        out_shape=[
            jax.ShapeDtypeStruct((rows, width), jnp.float32),
            jax.ShapeDtypeStruct((comps, cols), jnp.float32),
            jax.ShapeDtypeStruct((comps, width), jnp.float32),
        ],
        compiler_params=pltpu.CompilerParams(vmem_limit_bytes=LIMIT),
        name="first_pass",
    )(counts, mask_rows, loadings, test_matrix)


def second_kernel(share, counts_ref, mask_ref, load_ref, y_ref, z_ref, s_ref, d_ref, ga_ref):
    step = pl.program_id(0)
    masked = masked_rows(counts_ref, mask_ref, step)
    load = load_ref[...]
    sketch = y_ref[...] - dot(load, z_ref[...])
    s_ref[...] = sketch
    high, low = split(sketch)
    both = dot(jnp.concatenate([high, low], axis=1), masked, ((0,), (0,)), None)
    width = sketch.shape[1]
    part = both[:width] + both[width:]
    small = (
        dot(jnp.concatenate([sketch, load], axis=1), sketch, ((0,), (0,))) * share
    )

    @pl.when(step == 0)
    def _():
        d_ref[...] = part
        ga_ref[...] = small

    @pl.when(step > 0)
    def _():
        d_ref[...] += part
        ga_ref[...] += small


def second_pass(counts, mask_rows, loadings, y, z, share):
    rows, cols = counts.shape
    comps, width = loadings.shape[1], y.shape[1]
    return pl.pallas_call(
        functools.partial(second_kernel, share),
        grid=(rows // ROW_BLOCK,),
        in_specs=[
            pl.BlockSpec((ROW_BLOCK, cols), lambda i: (i, 0)),
            pl.BlockSpec(mask_rows.shape, lambda i: (0, 0, 0)),
            pl.BlockSpec((ROW_BLOCK, comps), lambda i: (i, 0)),
            pl.BlockSpec((ROW_BLOCK, width), lambda i: (i, 0)),
            pl.BlockSpec(z.shape, lambda i: (0, 0)),
        ],
        out_specs=[
            pl.BlockSpec((ROW_BLOCK, width), lambda i: (i, 0)),
            pl.BlockSpec((width, cols), lambda i: (0, 0)),
            pl.BlockSpec((width + comps, width), lambda i: (0, 0)),
        ],
        out_shape=[
            jax.ShapeDtypeStruct((rows, width), jnp.float32),
            jax.ShapeDtypeStruct((width, cols), jnp.float32),
            jax.ShapeDtypeStruct((width + comps, width), jnp.float32),
        ],
        compiler_params=pltpu.CompilerParams(vmem_limit_bytes=LIMIT),
        name="second_pass",
    )(counts, mask_rows, loadings, y, z)


class Group:
    def __init__(self, axis):
        self.axis = axis
        self.size = lax.axis_size(axis)
        self.me = lax.axis_index(axis)

    def peer(self, offset):
        return lax.rem(self.me + offset, self.size)

    def greet(self, barrier):
        for offset in range(1, self.size):
            pl.semaphore_signal(
                barrier, inc=1, device_id={self.axis: self.peer(offset)}, device_id_type=MESH
            )
        return self.size - 1

    def send(self, source, target, sems):
        copies = []
        for offset in range(1, self.size):
            peer = self.peer(offset)
            copy = pltpu.make_async_remote_copy(
                src_ref=source(peer),
                dst_ref=target,
                send_sem=sems.at[0, offset],
                recv_sem=sems.at[1, offset],
                device_id={self.axis: peer},
                device_id_type=MESH,
            )
            copy.start()
            copies.append(copy)
        return copies


def received(copies):
    for copy in copies:
        copy.wait_recv()


def sent(copies):
    for copy in copies:
        copy.wait_send()


def ordered_sum(slots, count):
    total = slots[0]
    for index in range(1, count):
        total = total + slots[index]
    return total


def rows_of(ref, index, count):
    return ref.at[pl.ds(pl.multiple_of(index * count, 8), count), :]


def cols_of(ref, index, count):
    return ref.at[:, pl.ds(pl.multiple_of(index * count, 128), count)]


def gather_kernel(
    y_in, p_in, z_in, y_out, p_out, z_out,
    z_cell, z_gene, p_slots, pair_slots, chip_slots,
    zc_sems, zg_sems, za_sems, p_sems, pair_sems, chip_sems, back_sems,
):
    gene, cell = Group("gene"), Group("cell")
    barrier = pltpu.get_barrier_semaphore()
    pl.semaphore_wait(barrier, gene.greet(barrier) + cell.greet(barrier))
    chips = cell.size // 2
    core = lax.rem(cell.me, 2)
    chip = cell.me // 2
    partner = cell.me + 1 - 2 * core
    rows = y_in.shape[0]
    half = rows // 2
    chunk = half // CHUNKS
    zrows = z_in.shape[0] // cell.size
    wide = p_in.shape[1] // gene.size

    def to(device, source, target, sems, *index):
        copy = pltpu.make_async_remote_copy(
            src_ref=source,
            dst_ref=target,
            send_sem=sems.at[(0,) + index],
            recv_sem=sems.at[(1,) + index],
            device_id={"cell": device},
            device_id_type=MESH,
        )
        copy.start()
        return copy

    pending = []
    z_first = cell.send(lambda q: rows_of(z_in, q, zrows), z_cell.at[cell.me], zc_sems)
    z_cell[cell.me] = rows_of(z_in, cell.me, zrows)[...]
    pairs = []
    for j in range(CHUNKS):
        start = pl.multiple_of((1 - core) * half + j * chunk, 8)
        pairs.append(
            to(partner, y_in.at[pl.ds(start, chunk), :],
               pair_slots.at[pl.ds(j * chunk, chunk), :], pair_sems, j)
        )
    received(z_first)
    z_gene[gene.me] = ordered_sum(z_cell, cell.size)
    z_second = gene.send(lambda q: z_gene.at[gene.me], z_gene.at[gene.me], zg_sems)
    p_copies = gene.send(lambda q: cols_of(p_in, q, wide), p_slots.at[gene.me], p_sems)
    p_slots[gene.me] = cols_of(p_in, gene.me, wide)[...]
    across = []
    for j in range(CHUNKS):
        start = pl.multiple_of(core * half + j * chunk, 8)
        pairs[j].wait_recv()
        span = pl.ds(j * chunk, chunk)
        chip_slots[chip, span, :] = y_in[pl.ds(start, chunk), :] + pair_slots[span, :]
        block = chip_slots.at[chip, span, :]
        for offset in range(1, chips):
            other = lax.rem(chip + offset, chips) * 2 + core
            across.append(to(other, block, block, chip_sems, offset, j))
    received(z_second)
    rows_of(z_out, cell.me, zrows)[...] = ordered_sum(z_gene, gene.size)
    block = rows_of(z_out, cell.me, zrows)
    z_third = cell.send(lambda q: block, block, za_sems)
    backs = []
    for j in range(CHUNKS):
        received(across[j * (chips - 1):(j + 1) * (chips - 1)])
        span = pl.ds(j * chunk, chunk)
        total = chip_slots[0, span, :]
        for index in range(1, chips):
            total = total + chip_slots[index, span, :]
        start = pl.multiple_of(core * half + j * chunk, 8)
        y_out[pl.ds(start, chunk), :] = total
        block = y_out.at[pl.ds(start, chunk), :]
        backs.append(to(partner, block, block, back_sems, j))
    received(z_third)
    received(p_copies)
    p_out[...] = ordered_sum(p_slots, gene.size)
    received(backs)
    sent(z_first + pairs + z_second + p_copies + across + z_third + backs)


def gather(y, p, z):
    genes, cells = lax.axis_size("gene"), lax.axis_size("cell")
    rows, width = y.shape
    comps, cols = p.shape
    dma = pltpu.SemaphoreType.DMA
    return pl.pallas_call(
        gather_kernel,
        in_specs=[VMEM] * 3,
        out_specs=[VMEM] * 3,
        out_shape=[
            jax.ShapeDtypeStruct(y.shape, jnp.float32),
            jax.ShapeDtypeStruct((comps, cols // genes), jnp.float32),
            jax.ShapeDtypeStruct(z.shape, jnp.float32),
        ],
        scratch_shapes=[
            pltpu.VMEM((cells, comps // cells, width), jnp.float32),
            pltpu.VMEM((genes, comps // cells, width), jnp.float32),
            pltpu.VMEM((genes, comps, cols // genes), jnp.float32),
            pltpu.VMEM((rows // 2, width), jnp.float32),
            pltpu.VMEM((cells // 2, rows // 2, width), jnp.float32),
            dma((2, cells)),
            dma((2, genes)),
            dma((2, cells)),
            dma((2, genes)),
            dma((2, CHUNKS)),
            dma((2, cells // 2, CHUNKS)),
            dma((2, CHUNKS)),
        ],
        compiler_params=pltpu.CompilerParams(
            collective_id=1, has_side_effects=True, vmem_limit_bytes=LIMIT
        ),
        name="gather",
    )(y, p, z)


def core_kernel(
    d_in, p_ref, ga_ref, out_ref,
    d_slots, parts, c_slots, g_slots,
    d_sems, c_sems, g_sems, ga_sems, ca_sems,
):
    gene, cell = Group("gene"), Group("cell")
    barrier = pltpu.get_barrier_semaphore()
    pl.semaphore_wait(barrier, gene.greet(barrier) + cell.greet(barrier))
    wide = d_in.shape[1] // gene.size
    d_copies = gene.send(lambda q: cols_of(d_in, q, wide), d_slots.at[gene.me], d_sems)
    d_slots[gene.me] = cols_of(d_in, gene.me, wide)[...]
    proj = p_ref[...]
    comps = proj.shape[0]
    width = d_in.shape[0]
    total_rows = parts.shape[0]
    small = 3 * comps + ga_ref.shape[0]
    parts[pl.ds(0, comps), :] = dot(proj, proj, ((1,), (1,)))
    parts[pl.ds(3 * comps, ga_ref.shape[0]), :] = ga_ref[...]
    if total_rows > small:
        parts[pl.ds(small, total_rows - small), :] = jnp.zeros(
            (total_rows - small, comps), jnp.float32
        )
    received(d_copies)
    inner = ordered_sum(d_slots, gene.size)
    parts[pl.ds(comps, comps), :] = dot(proj, inner, ((1,), (1,)))
    parts[pl.ds(2 * comps, width), :] = dot(inner, inner, ((1,), (1,)))
    c_rows = total_rows // cell.size
    g_rows = c_rows // gene.size
    first = cell.send(lambda q: rows_of(parts, q, c_rows), c_slots.at[cell.me], c_sems)
    c_slots[cell.me] = rows_of(parts, cell.me, c_rows)[...]
    received(first)
    sent(first)
    mine = rows_of(parts, cell.me, c_rows)
    mine[...] = ordered_sum(c_slots, cell.size)
    second = gene.send(lambda q: rows_of(mine, q, g_rows), g_slots.at[gene.me], g_sems)
    g_slots[gene.me] = rows_of(mine, gene.me, g_rows)[...]
    received(second)
    done = rows_of(rows_of(out_ref, cell.me, c_rows), gene.me, g_rows)
    done[...] = ordered_sum(g_slots, gene.size)
    third = gene.send(lambda q: done, done, ga_sems)
    received(third)
    block = rows_of(out_ref, cell.me, c_rows)
    fourth = cell.send(lambda q: block, block, ca_sems)
    received(fourth)
    sent(d_copies + second + third + fourth)


def core_sums(d, p, ga):
    genes, cells = lax.axis_size("gene"), lax.axis_size("cell")
    comps, wide = p.shape
    width = d.shape[0]
    unit = 8 * genes * cells
    total_rows = -(-(3 * comps + ga.shape[0]) // unit) * unit
    dma = pltpu.SemaphoreType.DMA
    return pl.pallas_call(
        core_kernel,
        in_specs=[VMEM] * 3,
        out_specs=VMEM,
        out_shape=jax.ShapeDtypeStruct((total_rows, comps), jnp.float32),
        scratch_shapes=[
            pltpu.VMEM((genes, width, wide), jnp.float32),
            pltpu.VMEM((total_rows, comps), jnp.float32),
            pltpu.VMEM((cells, total_rows // cells, comps), jnp.float32),
            pltpu.VMEM((genes, total_rows // cells // genes, comps), jnp.float32),
            dma((2, genes)),
            dma((2, cells)),
            dma((2, genes)),
            dma((2, genes)),
            dma((2, cells)),
        ],
        compiler_params=pltpu.CompilerParams(
            collective_id=2, has_side_effects=True, vmem_limit_bytes=LIMIT
        ),
        name="core_sums",
    )(d, p, ga)


def inverse_factor(gram):
    order = gram.shape[0]
    lane = lax.broadcasted_iota(jnp.int32, (1, order), 1)
    below = lax.broadcasted_iota(jnp.int32, (8, 1), 0)
    blocks = [gram[8 * b:8 * b + 8] for b in range(order // 8)]
    for k in range(order):
        home, spot = k // 8, k % 8
        pivot_row = blocks[home][spot:spot + 1]
        scaled = jnp.where(lane == k, 1.0, pivot_row) * (1.0 / pivot_row[:, k:k + 1])
        for b in range(home, order // 8):
            column = blocks[b][:, k:k + 1]
            kept = jnp.where(lane == k, 0.0, blocks[b])
            changed = kept - column * scaled
            if b == home:
                changed = jnp.where(below > spot, changed, blocks[b])
            blocks[b] = changed
    full = jnp.concatenate(blocks, axis=0)
    row = lax.broadcasted_iota(jnp.int32, (order, order), 0)
    col = lax.broadcasted_iota(jnp.int32, (order, order), 1)
    pivots = jnp.sum(jnp.where(row == col, full, 0.0), axis=1, keepdims=True)
    unit = jnp.where(col < row, full, jnp.where(col == row, 1.0, 0.0))
    return unit * lax.rsqrt(pivots)


def small_kernel(cells_total, sums_ref, values_ref, mix_ref, new_values_ref, core_ref, sub_ref, inv_ref):
    comps = values_ref.shape[1]
    pp = sums_ref[pl.ds(0, comps), :]
    pd = sums_ref[pl.ds(comps, comps), :]
    dd = sums_ref[pl.ds(2 * comps, comps), :]
    gram = sums_ref[pl.ds(3 * comps, comps), :]
    along_t = sums_ref[pl.ds(4 * comps, comps), :]
    inv_ref[...] = inverse_factor(gram)
    inv = inv_ref[...]
    cross = dot(pd, along_t, ((0,), (0,)))
    shifted = dot(pp, along_t)
    pc = dot(pd - shifted, inv, ((1,), (1,)))
    inner = dd - cross - cross.T + dot(along_t, shifted, ((0,), (0,)))
    cc = dot(dot(inv, inner), inv, ((1,), (1,)))
    row = lax.broadcasted_iota(jnp.int32, (comps, comps), 0)
    col = lax.broadcasted_iota(jnp.int32, (comps, comps), 1)
    values = values_ref[...]
    squares = jnp.where(row == col, values * values, 0.0)
    scale = 1.0 / cells_total
    core_ref[pl.ds(0, comps), pl.ds(0, comps)] = pp * scale + squares
    core_ref[pl.ds(0, comps), pl.ds(comps, comps)] = pc * scale
    core_ref[pl.ds(comps, comps), pl.ds(0, comps)] = pc.T * scale
    core_ref[pl.ds(comps, comps), pl.ds(comps, comps)] = cc * scale
    sub_ref[pl.ds(0, comps), :] = jnp.where(row == col, 1.0, 0.0)
    sub_ref[pl.ds(comps, comps), :] = jnp.zeros((comps, comps), jnp.float32)

    def sweep(index, carry):
        image = dot(core_ref[...], sub_ref[...])
        step = inverse_factor(dot(image, image, ((0,), (0,))))
        sub_ref[...] = dot(image, step, ((1,), (1,)))
        return carry

    lax.fori_loop(0, SWEEPS, sweep, 0)
    sub = sub_ref[...]
    image = dot(core_ref[...], sub)
    new_values_ref[...] = jnp.sqrt(jnp.sum(sub * image, axis=0, keepdims=True))
    mix_ref[pl.ds(0, comps), :] = sub[:comps]
    mix_ref[pl.ds(comps, comps), :] = dot(inv_ref[...], sub[comps:], ((0,), (0,)))


def small(sums, values, cells_total):
    comps = values.shape[0]
    return pl.pallas_call(
        functools.partial(small_kernel, cells_total),
        in_specs=[VMEM] * 2,
        out_specs=[VMEM] * 2,
        out_shape=[
            jax.ShapeDtypeStruct((2 * comps, comps), jnp.float32),
            jax.ShapeDtypeStruct((1, comps), jnp.float32),
        ],
        scratch_shapes=[
            pltpu.VMEM((2 * comps, 2 * comps), jnp.float32),
            pltpu.VMEM((2 * comps, comps), jnp.float32),
            pltpu.VMEM((comps, comps), jnp.float32),
        ],
        name="small",
    )(sums, values.reshape(1, comps))


def local(counts, loadings, values, test_matrix, tile_mask):
    gene_rows, cell_cols = counts.shape
    comps = loadings.shape[1]
    genes_total = gene_rows * lax.axis_size("gene")
    cells = lax.axis_size("cell")
    mask_rows = jnp.repeat(tile_mask.astype(jnp.float32), CELL_TILE, axis=1)[:, None, :]
    y, p, z = first_pass(counts, mask_rows, loadings, test_matrix)
    y, p, z = gather(y, p, z)
    sketch, d, ga = second_pass(counts, mask_rows, loadings, y, z, 1.0 / cells)
    sums = core_sums(d, p, ga)
    mix, new_values = small(sums, values, cell_cols * cells)
    root = genes_total**0.5
    rotated = jnp.dot(loadings, mix[:comps], precision=HIGH) + jnp.dot(
        sketch, mix[comps:], precision=HIGH
    )
    return rotated * root, new_values.reshape(comps)


def solution(mesh):
    placed = (P("gene", "cell"), P("gene", None), P(), P("cell", None), P("gene", "cell"))
    return jax.shard_map(
        local, mesh=mesh, in_specs=placed, out_specs=(P("gene", None), P()), check_vma=False
    )
```

```python
import functools

import jax
import jax.numpy as jnp
from jax import lax
from jax.experimental import pallas as pl
from jax.experimental.pallas import tpu as pltpu
from jax.sharding import PartitionSpec as P

GENE_TILE = 256
CELL_TILE = 128
SWEEPS = 3
ROW_BLOCK = 512
CHUNKS = 8
HIGH = lax.Precision.HIGHEST
GROUP = 8
MESH = pl.DeviceIdType.MESH
LIMIT = 60 * 1024 * 1024
VMEM = pl.BlockSpec(memory_space=pltpu.VMEM)


def dot(a, b, dims=((1,), (0,)), precision=HIGH):
    return lax.dot_general(
        a, b, (dims, ((), ())), precision=precision, preferred_element_type=jnp.float32
    )


def split(a):
    high = a.astype(jnp.bfloat16)
    return high, (a - high.astype(jnp.float32)).astype(jnp.bfloat16)


def dot_split(a, b):
    return (
        dot(a[0], b[0], precision=None)
        + dot(a[0], b[1], precision=None)
        + dot(a[1], b[0], precision=None)
    )


def masked_rows(counts_ref, mask_ref, step):
    parts = []
    per_block = ROW_BLOCK // GENE_TILE
    for part in range(per_block):
        row = mask_ref[step * per_block + part].astype(jnp.bfloat16)
        parts.append(counts_ref[pl.ds(part * GENE_TILE, GENE_TILE), :] * row)
    return jnp.concatenate(parts, axis=0)


def first_kernel(counts_ref, mask_ref, load_ref, test_ref, y_ref, p_ref, z_ref):
    step = pl.program_id(0)
    masked = masked_rows(counts_ref, mask_ref, step)
    y_ref[...] = dot(masked, test_ref[...], precision=None)
    part = dot(load_ref[...].astype(jnp.bfloat16), masked, ((0,), (0,)), None)

    @pl.when(step == 0)
    def _():
        p_ref[...] = part

    @pl.when(step > 0)
    def _():
        p_ref[...] += part

    @pl.when(step == pl.num_programs(0) - 1)
    def _():
        high, low = split(p_ref[...])
        z_ref[...] = dot(high, test_ref[...], precision=None) + dot(
            low, test_ref[...], precision=None
        )


def first_pass(counts, mask_rows, loadings, test_matrix):
    rows, cols = counts.shape
    comps, width = loadings.shape[1], test_matrix.shape[1]
    return pl.pallas_call(
        first_kernel,
        grid=(rows // ROW_BLOCK,),
        in_specs=[
            pl.BlockSpec((ROW_BLOCK, cols), lambda i: (i, 0)),
            pl.BlockSpec(mask_rows.shape, lambda i: (0, 0, 0)),
            pl.BlockSpec((ROW_BLOCK, comps), lambda i: (i, 0)),
            pl.BlockSpec(test_matrix.shape, lambda i: (0, 0)),
        ],
        out_specs=[
            pl.BlockSpec((ROW_BLOCK, width), lambda i: (i, 0)),
            pl.BlockSpec((comps, cols), lambda i: (0, 0)),
            pl.BlockSpec((comps, width), lambda i: (0, 0)),
        ],
        out_shape=[
            jax.ShapeDtypeStruct((rows, width), jnp.float32),
            jax.ShapeDtypeStruct((comps, cols), jnp.float32),
            jax.ShapeDtypeStruct((comps, width), jnp.float32),
        ],
        compiler_params=pltpu.CompilerParams(vmem_limit_bytes=LIMIT),
        name="first_pass",
    )(counts, mask_rows, loadings, test_matrix)


def second_kernel(steps, counts_ref, mask_ref, load_ref, y_ref, z_ref, s_ref, d_ref, ga_ref):
    step = pl.program_id(0)
    masked = masked_rows(counts_ref, mask_ref, step)
    load = load_ref[...]
    sketch = y_ref[...] - dot_split(split(load), split(z_ref[...]))
    s_ref[...] = sketch
    high, low = split(sketch)
    both = dot(jnp.concatenate([high, low], axis=1), masked, ((0,), (0,)), None)
    width = sketch.shape[1]
    part = both[:width] + both[width:]

    @pl.when(step == 0)
    def _():
        d_ref[...] = part
        ga_ref[...] = jnp.zeros_like(ga_ref)

    @pl.when(step > 0)
    def _():
        d_ref[...] += part

    cells = lax.axis_size("cell")
    every = pl.cdiv(steps, cells)

    @pl.when(step // every == lax.axis_index("cell"))
    def _():
        ga_ref[...] += dot(jnp.concatenate([sketch, load], axis=1), sketch, ((0,), (0,)))


def second_pass(counts, mask_rows, loadings, y, z):
    rows, cols = counts.shape
    comps, width = loadings.shape[1], y.shape[1]
    return pl.pallas_call(
        functools.partial(second_kernel, rows // ROW_BLOCK),
        grid=(rows // ROW_BLOCK,),
        in_specs=[
            pl.BlockSpec((ROW_BLOCK, cols), lambda i: (i, 0)),
            pl.BlockSpec(mask_rows.shape, lambda i: (0, 0, 0)),
            pl.BlockSpec((ROW_BLOCK, comps), lambda i: (i, 0)),
            pl.BlockSpec((ROW_BLOCK, width), lambda i: (i, 0)),
            pl.BlockSpec(z.shape, lambda i: (0, 0)),
        ],
        out_specs=[
            pl.BlockSpec((ROW_BLOCK, width), lambda i: (i, 0)),
            pl.BlockSpec((width, cols), lambda i: (0, 0)),
            pl.BlockSpec((width + comps, width), lambda i: (0, 0)),
        ],
        out_shape=[
            jax.ShapeDtypeStruct((rows, width), jnp.float32),
            jax.ShapeDtypeStruct((width, cols), jnp.float32),
            jax.ShapeDtypeStruct((width + comps, width), jnp.float32),
        ],
        compiler_params=pltpu.CompilerParams(vmem_limit_bytes=LIMIT),
        name="second_pass",
    )(counts, mask_rows, loadings, y, z)


class Group:
    def __init__(self, axis):
        self.axis = axis
        self.size = lax.axis_size(axis)
        self.me = lax.axis_index(axis)

    def peer(self, offset):
        return lax.rem(self.me + offset, self.size)

    def greet(self, barrier):
        for offset in range(1, self.size):
            pl.semaphore_signal(
                barrier, inc=1, device_id={self.axis: self.peer(offset)}, device_id_type=MESH
            )
        return self.size - 1

    def send(self, source, target, sems):
        copies = []
        for offset in range(1, self.size):
            peer = self.peer(offset)
            copy = pltpu.make_async_remote_copy(
                src_ref=source(peer),
                dst_ref=target,
                send_sem=sems.at[0, offset],
                recv_sem=sems.at[1, offset],
                device_id={self.axis: peer},
                device_id_type=MESH,
            )
            copy.start()
            copies.append(copy)
        return copies


def received(copies):
    for copy in copies:
        copy.wait_recv()


def sent(copies):
    for copy in copies:
        copy.wait_send()


def ordered_sum(slots, count):
    total = slots[0]
    for index in range(1, count):
        total = total + slots[index]
    return total


def rows_of(ref, index, count):
    return ref.at[pl.ds(pl.multiple_of(index * count, 8), count), :]


def cols_of(ref, index, count):
    return ref.at[:, pl.ds(pl.multiple_of(index * count, 128), count)]


class Scatter:
    def __init__(self, gene, source, pair_slots, slots, pair_sems, sems):
        self.gene, self.source = gene, source
        self.pair_slots, self.slots = pair_slots, slots
        self.pair_sems, self.sems = pair_sems, sems
        self.wide = source.shape[1] // gene.size
        self.half = gene.size // 2
        self.parity = lax.rem(gene.me, 2)
        self.place = gene.me // 2
        self.owners = [lax.rem(self.place + 1 + o, self.half) for o in range(self.half)]

    def copy(self, source, target, sems, index, device):
        copy = pltpu.make_async_remote_copy(
            src_ref=source,
            dst_ref=target,
            send_sem=sems.at[0, index],
            recv_sem=sems.at[1, index],
            device_id={"gene": device},
            device_id_type=MESH,
        )
        copy.start()
        return copy

    def start(self):
        partner = self.gene.me + 1 - 2 * self.parity
        self.pairs = [
            self.copy(
                cols_of(self.source, 2 * q + 1 - self.parity, self.wide),
                self.pair_slots.at[q], self.pair_sems, o, partner,
            )
            for o, q in enumerate(self.owners)
        ]

    def relay(self):
        self.across = []
        for o, q in enumerate(self.owners):
            self.pairs[o].wait_recv()
            own = 2 * q + self.parity
            total = cols_of(self.source, own, self.wide)[...] + self.pair_slots[q]
            if o == self.half - 1:
                self.slots[q] = total
            else:
                self.pair_slots[q] = total
                self.across.append(
                    self.copy(
                        self.pair_slots.at[q], self.slots.at[self.place], self.sems, o, own
                    )
                )

    def finish(self):
        received(self.across)
        return ordered_sum(self.slots, self.half)

    def sent(self):
        sent(self.pairs + self.across)


class AllSum:
    def __init__(self, gene, cell, parts, out, c_slots, g_slots, sems):
        self.gene, self.cell, self.parts, self.out = gene, cell, parts, out
        self.c_slots, self.g_slots, self.sems = c_slots, g_slots, sems
        self.c_rows = parts.shape[0] // cell.size
        self.g_rows = self.c_rows // gene.size

    def start(self):
        cell = self.cell
        self.first = cell.send(
            lambda q: rows_of(self.parts, q, self.c_rows), self.c_slots.at[cell.me], self.sems[0]
        )
        self.c_slots[cell.me] = rows_of(self.parts, cell.me, self.c_rows)[...]

    def over_gene(self):
        gene, cell = self.gene, self.cell
        received(self.first)
        sent(self.first)
        mine = rows_of(self.parts, cell.me, self.c_rows)
        mine[...] = ordered_sum(self.c_slots, cell.size)
        self.second = gene.send(
            lambda q: rows_of(mine, q, self.g_rows), self.g_slots.at[gene.me], self.sems[1]
        )
        self.g_slots[gene.me] = rows_of(mine, gene.me, self.g_rows)[...]

    def back_gene(self):
        gene, cell = self.gene, self.cell
        received(self.second)
        done = rows_of(rows_of(self.out, cell.me, self.c_rows), gene.me, self.g_rows)
        done[...] = ordered_sum(self.g_slots, gene.size)
        self.third = gene.send(lambda q: done, done, self.sems[2])

    def back_cell(self):
        received(self.third)
        block = rows_of(self.out, self.cell.me, self.c_rows)
        self.fourth = self.cell.send(lambda q: block, block, self.sems[3])

    def finish(self):
        received(self.fourth)
        sent(self.second + self.third + self.fourth)


def gather_kernel(
    y_in, p_in, z_in, y_out, p_out, z_out,
    z_cell, z_gene, p_pairs, p_slots, pair_slots, chip_slots,
    zc_sems, zg_sems, za_sems, pp_sems, p_sems, pair_sems, chip_sems, back_sems,
):
    gene, cell = Group("gene"), Group("cell")
    barrier = pltpu.get_barrier_semaphore()
    pl.semaphore_wait(barrier, gene.greet(barrier) + cell.greet(barrier))
    chips = cell.size // 2
    core = lax.rem(cell.me, 2)
    chip = cell.me // 2
    partner = cell.me + 1 - 2 * core
    rows = y_in.shape[0]
    half = rows // 2
    chunk = half // CHUNKS
    zrows = z_in.shape[0] // cell.size
    scatter = Scatter(gene, p_in, p_pairs, p_slots, pp_sems, p_sems)

    def to(device, source, target, sems, *index):
        copy = pltpu.make_async_remote_copy(
            src_ref=source,
            dst_ref=target,
            send_sem=sems.at[(0,) + index],
            recv_sem=sems.at[(1,) + index],
            device_id={"cell": device},
            device_id_type=MESH,
        )
        copy.start()
        return copy

    z_first = cell.send(lambda q: rows_of(z_in, q, zrows), z_cell.at[cell.me], zc_sems)
    z_cell[cell.me] = rows_of(z_in, cell.me, zrows)[...]
    pairs = []
    for j in range(CHUNKS):
        start = pl.multiple_of((1 - core) * half + j * chunk, 8)
        pairs.append(
            to(partner, y_in.at[pl.ds(start, chunk), :],
               pair_slots.at[pl.ds(j * chunk, chunk), :], pair_sems, j)
        )
    received(z_first)
    z_gene[gene.me] = ordered_sum(z_cell, cell.size)
    z_second = gene.send(lambda q: z_gene.at[gene.me], z_gene.at[gene.me], zg_sems)
    scatter.start()
    across = []
    for j in range(CHUNKS):
        start = pl.multiple_of(core * half + j * chunk, 8)
        pairs[j].wait_recv()
        span = pl.ds(j * chunk, chunk)
        chip_slots[chip, span, :] = y_in[pl.ds(start, chunk), :] + pair_slots[span, :]
        block = chip_slots.at[chip, span, :]
        for offset in range(1, chips):
            other = lax.rem(chip + offset, chips) * 2 + core
            across.append(to(other, block, block, chip_sems, offset, j))
    scatter.relay()
    received(z_second)
    rows_of(z_out, cell.me, zrows)[...] = ordered_sum(z_gene, gene.size)
    block = rows_of(z_out, cell.me, zrows)
    z_third = cell.send(lambda q: block, block, za_sems)
    backs = []
    for j in range(CHUNKS):
        received(across[j * (chips - 1):(j + 1) * (chips - 1)])
        span = pl.ds(j * chunk, chunk)
        total = chip_slots[0, span, :]
        for index in range(1, chips):
            total = total + chip_slots[index, span, :]
        start = pl.multiple_of(core * half + j * chunk, 8)
        y_out[pl.ds(start, chunk), :] = total
        block = y_out.at[pl.ds(start, chunk), :]
        backs.append(to(partner, block, block, back_sems, j))
    received(z_third)
    p_out[...] = scatter.finish()
    received(backs)
    scatter.sent()
    sent(z_first + pairs + z_second + across + z_third + backs)


def gather(y, p, z):
    genes, cells = lax.axis_size("gene"), lax.axis_size("cell")
    rows, width = y.shape
    comps, cols = p.shape
    dma = pltpu.SemaphoreType.DMA
    return pl.pallas_call(
        gather_kernel,
        in_specs=[VMEM] * 3,
        out_specs=[VMEM] * 3,
        out_shape=[
            jax.ShapeDtypeStruct(y.shape, jnp.float32),
            jax.ShapeDtypeStruct((comps, cols // genes), jnp.float32),
            jax.ShapeDtypeStruct(z.shape, jnp.float32),
        ],
        scratch_shapes=[
            pltpu.VMEM((cells, comps // cells, width), jnp.float32),
            pltpu.VMEM((genes, comps // cells, width), jnp.float32),
            pltpu.VMEM((genes // 2, comps, cols // genes), jnp.float32),
            pltpu.VMEM((genes // 2, comps, cols // genes), jnp.float32),
            pltpu.VMEM((rows // 2, width), jnp.float32),
            pltpu.VMEM((cells // 2, rows // 2, width), jnp.float32),
            dma((2, cells)),
            dma((2, genes)),
            dma((2, cells)),
            dma((2, genes // 2)),
            dma((2, genes // 2)),
            dma((2, CHUNKS)),
            dma((2, cells // 2, CHUNKS)),
            dma((2, CHUNKS)),
        ],
        compiler_params=pltpu.CompilerParams(
            collective_id=1, has_side_effects=True, vmem_limit_bytes=LIMIT
        ),
        name="gather",
    )(y, p, z)


def core_kernel(
    d_in, p_ref, ga_ref, early_out, late_out,
    d_pairs, d_slots, early, late, ec_slots, eg_slots, lc_slots, lg_slots,
    pair_sems, d_sems, *sems,
):
    gene, cell = Group("gene"), Group("cell")
    barrier = pltpu.get_barrier_semaphore()
    pl.semaphore_wait(barrier, gene.greet(barrier) + cell.greet(barrier))
    scatter = Scatter(gene, d_in, d_pairs, d_slots, pair_sems, d_sems)
    scatter.start()
    proj = p_ref[...]
    comps = proj.shape[0]
    small = ga_ref.shape[0]
    early[pl.ds(0, comps), :] = dot(proj, proj, ((1,), (1,)))
    early[pl.ds(comps, small), :] = ga_ref[...]
    for ref, used in ((early, comps + small), (late, 2 * comps)):
        rest = ref.shape[0] - used
        if rest:
            ref[pl.ds(used, rest), :] = jnp.zeros((rest, comps), jnp.float32)
    first = AllSum(gene, cell, early, early_out, ec_slots, eg_slots, sems[:4])
    second = AllSum(gene, cell, late, late_out, lc_slots, lg_slots, sems[4:])
    first.start()
    scatter.relay()
    first.over_gene()
    inner = scatter.finish()
    late[pl.ds(0, comps), :] = dot(proj, inner, ((1,), (1,)))
    late[pl.ds(comps, comps), :] = dot(inner, inner, ((1,), (1,)))
    second.start()
    first.back_gene()
    second.over_gene()
    first.back_cell()
    second.back_gene()
    second.back_cell()
    first.finish()
    second.finish()
    scatter.sent()


def core_sums(d, p, ga):
    genes, cells = lax.axis_size("gene"), lax.axis_size("cell")
    comps, wide = p.shape
    width = d.shape[0]
    unit = 8 * genes * cells
    early = -(-(comps + ga.shape[0]) // unit) * unit
    late = -(-(2 * comps) // unit) * unit
    dma = pltpu.SemaphoreType.DMA

    def slots(rows):
        return [
            pltpu.VMEM((cells, rows // cells, comps), jnp.float32),
            pltpu.VMEM((genes, rows // cells // genes, comps), jnp.float32),
        ]

    sems = [dma((2, cells)), dma((2, genes)), dma((2, genes)), dma((2, cells))]
    return pl.pallas_call(
        core_kernel,
        in_specs=[VMEM] * 3,
        out_specs=[VMEM] * 2,
        out_shape=[
            jax.ShapeDtypeStruct((early, comps), jnp.float32),
            jax.ShapeDtypeStruct((late, comps), jnp.float32),
        ],
        scratch_shapes=[
            pltpu.VMEM((genes // 2, width, wide), jnp.float32),
            pltpu.VMEM((genes // 2, width, wide), jnp.float32),
            pltpu.VMEM((early, comps), jnp.float32),
            pltpu.VMEM((late, comps), jnp.float32),
            *slots(early),
            *slots(late),
            dma((2, genes // 2)),
            dma((2, genes // 2)),
            *sems,
            *sems,
        ],
        compiler_params=pltpu.CompilerParams(
            collective_id=2, has_side_effects=True, vmem_limit_bytes=LIMIT
        ),
        name="core_sums",
    )(d, p, ga)


def inverse_factor(gram):
    order = gram.shape[0]
    shape = (8, order)
    lane = lax.broadcasted_iota(jnp.int32, shape, 1)
    sub = lax.broadcasted_iota(jnp.int32, shape, 0)
    count = order // 8
    blocks = [gram[8 * b:8 * b + 8] for b in range(count)]
    for k in range(0, order, GROUP):
        home, spot = k // 8, k % 8
        last = k + GROUP - 1
        columns = {
            b: [jnp.broadcast_to(blocks[b][:, k + i:k + i + 1], shape) for i in range(GROUP)]
            for b in range(home, count)
        }
        rows = [
            jnp.broadcast_to(blocks[home][spot + i:spot + i + 1], shape) for i in range(GROUP)
        ]
        entry = [
            [jnp.broadcast_to(rows[i][:, k + j:k + j + 1], shape) for j in range(GROUP)]
            for i in range(GROUP)
        ]
        scaled = []
        for i in range(GROUP):
            inverse = 1.0 / entry[i][i]
            row = jnp.where(lane == k + i, 1.0, rows[i]) * inverse
            ratio = [entry[i][m] * inverse for m in range(GROUP)]
            for j in range(i + 1, GROUP):
                rows[j] = jnp.where(lane == k + i, 0.0, rows[j]) - entry[j][i] * row
                for m in range(i + 1, GROUP):
                    entry[j][m] = entry[j][m] - entry[j][i] * ratio[m]
            for b in range(home, count):
                for m in range(i + 1, GROUP):
                    columns[b][m] = columns[b][m] - columns[b][i] * ratio[m]
            scaled.append(jnp.where((lane > k + i) & (lane <= last), 0.0, row))
        inside = (lane >= k) & (lane <= last)
        for b in range(home, count):
            if b == home and spot + GROUP == 8:
                changed = blocks[b]
            else:
                changed = jnp.where(inside, 0.0, blocks[b])
                for i in range(GROUP):
                    changed = changed - columns[b][i] * scaled[i]
            if b == home:
                changed = jnp.where(sub < spot, blocks[b], changed)
                for i in range(GROUP):
                    changed = jnp.where(sub == spot + i, rows[i], changed)
            blocks[b] = changed
    full = jnp.concatenate(blocks, axis=0)
    row = lax.broadcasted_iota(jnp.int32, (order, order), 0)
    col = lax.broadcasted_iota(jnp.int32, (order, order), 1)
    pivots = jnp.sum(jnp.where(row == col, full, 0.0), axis=1, keepdims=True)
    unit = jnp.where(col < row, full, jnp.where(col == row, 1.0, 0.0))
    return unit * lax.rsqrt(pivots)


def small_kernel(
    cells_total, root, early_ref, late_ref, values_ref,
    mix_ref, new_values_ref, core_ref, sub_ref, inv_ref,
):
    comps = values_ref.shape[1]
    pp = early_ref[pl.ds(0, comps), :]
    gram = early_ref[pl.ds(comps, comps), :]
    along_t = early_ref[pl.ds(2 * comps, comps), :]
    pd = late_ref[pl.ds(0, comps), :]
    dd = late_ref[pl.ds(comps, comps), :]
    inv_ref[...] = inverse_factor(gram)
    inv = inv_ref[...]
    cross = dot(pd, along_t, ((0,), (0,)))
    shifted = dot(pp, along_t)
    pc = dot(pd - shifted, inv, ((1,), (1,)))
    inner = dd - cross - cross.T + dot(along_t, shifted, ((0,), (0,)))
    cc = dot(dot(inv, inner), inv, ((1,), (1,)))
    row = lax.broadcasted_iota(jnp.int32, (comps, comps), 0)
    col = lax.broadcasted_iota(jnp.int32, (comps, comps), 1)
    values = values_ref[...]
    squares = jnp.where(row == col, values * values, 0.0)
    scale = 1.0 / cells_total
    core_ref[pl.ds(0, comps), pl.ds(0, comps)] = pp * scale + squares
    core_ref[pl.ds(0, comps), pl.ds(comps, comps)] = pc * scale
    core_ref[pl.ds(comps, comps), pl.ds(0, comps)] = pc.T * scale
    core_ref[pl.ds(comps, comps), pl.ds(comps, comps)] = cc * scale
    sub_ref[pl.ds(0, comps), :] = jnp.where(row == col, 1.0, 0.0)
    sub_ref[pl.ds(comps, comps), :] = jnp.zeros((comps, comps), jnp.float32)

    def sweep(index, carry):
        image = dot(core_ref[...], sub_ref[...])
        step = inverse_factor(dot(image, image, ((0,), (0,))))
        sub_ref[...] = dot(image, step, ((1,), (1,)))
        return carry

    lax.fori_loop(0, SWEEPS, sweep, 0)
    sub = sub_ref[...]
    image = dot(core_ref[...], sub)
    new_values_ref[...] = jnp.sqrt(jnp.sum(sub * image, axis=0, keepdims=True))
    mix_ref[pl.ds(0, comps), :] = sub[:comps] * root
    mix_ref[pl.ds(comps, comps), :] = dot(inv_ref[...], sub[comps:], ((0,), (0,))) * root


def small(early, late, values, cells_total, root):
    comps = values.shape[0]
    return pl.pallas_call(
        functools.partial(small_kernel, cells_total, root),
        in_specs=[VMEM] * 3,
        out_specs=[VMEM] * 2,
        out_shape=[
            jax.ShapeDtypeStruct((2 * comps, comps), jnp.float32),
            jax.ShapeDtypeStruct((1, comps), jnp.float32),
        ],
        scratch_shapes=[
            pltpu.VMEM((2 * comps, 2 * comps), jnp.float32),
            pltpu.VMEM((2 * comps, comps), jnp.float32),
            pltpu.VMEM((comps, comps), jnp.float32),
        ],
        name="small",
    )(early, late, values.reshape(1, comps))


def last_kernel(load_ref, sketch_ref, mix_ref, out_ref):
    both = jnp.concatenate([load_ref[...], sketch_ref[...]], axis=1)
    out_ref[...] = dot_split(split(both), split(mix_ref[...]))


def last_pass(loadings, sketch, mix):
    rows, comps = loadings.shape
    block = pl.BlockSpec((2 * ROW_BLOCK, comps), lambda i: (i, 0))
    return pl.pallas_call(
        last_kernel,
        grid=(rows // (2 * ROW_BLOCK),),
        in_specs=[block, block, pl.BlockSpec(mix.shape, lambda i: (0, 0))],
        out_specs=block,
        out_shape=jax.ShapeDtypeStruct((rows, comps), jnp.float32),
        name="last_pass",
    )(loadings, sketch, mix)


def local(counts, loadings, values, test_matrix, tile_mask):
    gene_rows, cell_cols = counts.shape
    comps = loadings.shape[1]
    genes_total = gene_rows * lax.axis_size("gene")
    cells = lax.axis_size("cell")
    mask_rows = jnp.repeat(tile_mask.astype(jnp.float32), CELL_TILE, axis=1)[:, None, :]
    y, p, z = first_pass(counts, mask_rows, loadings, test_matrix)
    y, p, z = gather(y, p, z)
    sketch, d, ga = second_pass(counts, mask_rows, loadings, y, z)
    early, late = core_sums(d, p, ga)
    mix, new_values = small(early, late, values, cell_cols * cells, genes_total**0.5)
    return last_pass(loadings, sketch, mix), new_values.reshape(comps)


def solution(mesh):
    placed = (P("gene", "cell"), P("gene", None), P(), P("cell", None), P("gene", "cell"))
    return jax.shard_map(
        local, mesh=mesh, in_specs=placed, out_specs=(P("gene", None), P()), check_vma=False
    )
```
